32 devices in a mesh: gx: 4 (over z), gy: 4 (over x, core), gz: 2 (over y).
Axes of the slice: x: 2, y: 2, z: 4, core: 2. Of those that a mesh axis runs over, the one named last changes fastest.
Arguments:
- residual: float32 [32, 32, 256], P('gx', 'gy', 'gz'), may hold values from -18 to 18
- direction: float32 [32, 32, 256], P('gx', 'gy', 'gz'), may hold values from -18 to 18
Outputs:
- powers: float32 [2, 4, 32, 32, 256], P(None, None, 'gx', 'gy', 'gz')
- gram_matrix: float32 [9, 9], replicated
- projections: float32 [9], replicated
The draws below stay inside these ranges and needn't reach their ends.
All inputs are finite; a program needn't handle non-finite values.
Results may differ from the reference program's by a relative error of at most 0.00029.
Values sent between devices are 32-bit elements; how exact they have to be, the bound alone decides.
A program may use at most 64 MiB of HBM per device.

```python
import jax
import jax.numpy as jnp

STEPS = 4
MARGIN = 1
SWEEPS = 3
NX = 32
NY = 32
NZ = 256
N_GX = 4
N_GY = 4
N_GZ = 2


def cell_law(key, salt):
    shape_cells = (NX, NY, NZ)
    gaussian = jnp.clip(jax.random.normal(jax.random.fold_in(key, salt), shape_cells, jnp.float32), -4.0, 4.0)
    levels = jax.random.uniform(jax.random.fold_in(key, salt + 1), shape_cells, jnp.float32)
    spread = 0.3 * jnp.exp(levels * jnp.log(10.0))
    along_x = jnp.arange(NX, dtype=jnp.float32) / max(NX - 1, 1)
    ramped = 0.5 + along_x
    return gaussian * spread * ramped[:, None, None]


def draw_residual(key, part):
    return cell_law(key, 1)


def draw_direction(key, part):
    return cell_law(key, 5)


def setup_inputs(seed: int = 0) -> dict:
    arg_keys = jax.random.split(jax.random.key(seed), 3)
    residual = draw_residual(jax.random.fold_in(arg_keys[2], 71), 0)
    direction = draw_direction(jax.random.fold_in(arg_keys[2], 71), 0)
    return dict(residual=residual, direction=direction)


SWEEP_SCALE = 1.0 / 9.0


def grid_operator(values):
    padded = jnp.pad(values, 1)
    center = padded[1:-1, 1:-1, 1:-1]
    beside = padded[2:, 1:-1, 1:-1] + padded[:-2, 1:-1, 1:-1]
    beside = beside + padded[1:-1, 2:, 1:-1] + padded[1:-1, :-2, 1:-1]
    beside = beside + padded[1:-1, 1:-1, 2:] + padded[1:-1, 1:-1, :-2]
    return 6.0 * center - beside


def block_operator(values):
    padded = jnp.pad(values, [(0, 0), (1, 1), (0, 0), (1, 1), (0, 0), (1, 1)])
    center = padded[:, 1:-1, :, 1:-1, :, 1:-1]
    beside = padded[:, 2:, :, 1:-1, :, 1:-1] + padded[:, :-2, :, 1:-1, :, 1:-1]
    beside = beside + padded[:, 1:-1, :, 2:, :, 1:-1] + padded[:, 1:-1, :, :-2, :, 1:-1]
    beside = beside + padded[:, 1:-1, :, 1:-1, :, 2:] + padded[:, 1:-1, :, 1:-1, :, :-2]
    return 6.0 * center - beside


def extend_axis(values, position, blocks, margin):
    leading = jnp.moveaxis(values, position, 0)
    length = leading.shape[0]
    block_width = length // blocks
    trailing = leading.shape[1:]
    padded = jnp.pad(leading, [(margin, margin)] + [(0, 0)] * len(trailing))
    below_part = padded[0:length].reshape((blocks, block_width) + trailing)[:, :margin]
    middle = leading.reshape((blocks, block_width) + trailing)
    above_part = padded[2 * margin:2 * margin + length].reshape((blocks, block_width) + trailing)[:, block_width - margin:]
    joined = jnp.concatenate([below_part, middle, above_part], axis=1)
    return jnp.moveaxis(joined, (0, 1), (position, position + 1))


def fold_axis(values, position, margin):
    leading = jnp.moveaxis(values, (position, position + 1), (0, 1))
    blocks = leading.shape[0]
    block_width = leading.shape[1] - 2 * margin
    trailing = leading.shape[2:]
    length = blocks * block_width
    zero_tail = [(0, 0)] * len(trailing)
    middle = leading[:, margin:margin + block_width].reshape((length,) + trailing)
    below_part = jnp.pad(leading[:, :margin], [(0, 0), (0, block_width - margin)] + zero_tail).reshape((length,) + trailing)
    above_part = jnp.pad(leading[:, block_width + margin:], [(0, 0), (block_width - margin, 0)] + zero_tail).reshape((length,) + trailing)
    combined = jnp.pad(middle, [(margin, margin)] + zero_tail)
    combined = combined + jnp.pad(below_part, [(0, 2 * margin)] + zero_tail)
    combined = combined + jnp.pad(above_part, [(2 * margin, 0)] + zero_tail)
    return jnp.moveaxis(combined[margin:margin + length], 0, position)


def extend_grid(values):
    values = extend_axis(values, 0, N_GX, MARGIN)
    values = extend_axis(values, 2, N_GY, MARGIN)
    return extend_axis(values, 4, N_GZ, MARGIN)


def fold_grid(values):
    values = fold_axis(values, 4, MARGIN)
    values = fold_axis(values, 2, MARGIN)
    return fold_axis(values, 0, MARGIN)


def precondition(values, mask):
    source = mask * extend_grid(values)
    iterate = mask * (SWEEP_SCALE * source)
    for sweep_index in range(SWEEPS - 1):
        iterate = mask * (iterate + SWEEP_SCALE * (source - block_operator(iterate)))
    return fold_grid(iterate)


def reference(residual, direction):
    mask = extend_grid(jnp.ones(residual.shape, jnp.float32))
    cell_count = NX * NY * NZ
    p_fields = [direction]
    p_images = []
    for step_index in range(STEPS):
        p_images.append(grid_operator(p_fields[-1]))
        p_fields.append(precondition(p_images[-1], mask))
    p_images.append(grid_operator(p_fields[-1]))
    z_fields = [precondition(residual, mask)]
    z_images = []
    for step_index in range(STEPS - 1):
        z_images.append(grid_operator(z_fields[-1]))
        z_fields.append(precondition(z_images[-1], mask))
    z_images.append(grid_operator(z_fields[-1]))
    basis = p_fields + z_fields
    images = p_images + z_images
    table_rows = []
    for left_field in basis:
        table_rows.append(jnp.stack([jnp.sum(left_field * right_image) for right_image in images]))
    gram_matrix = jnp.stack(table_rows) / cell_count
    projections = jnp.stack([jnp.sum(left_field * residual) for left_field in basis]) / cell_count
    powers = jnp.stack([jnp.stack(p_fields[1:]), jnp.stack(z_fields)])
    return (powers, gram_matrix, projections)
```

```python
import functools

import jax
import jax.numpy as jnp
from jax import lax
from jax.experimental import pallas as pl
from jax.experimental.pallas import tpu as pltpu
from jax.sharding import PartitionSpec as P

STEPS = 4
SWEEPS = 3
LANES = 128
MESH = pl.DeviceIdType.MESH
HIGHEST = lax.Precision.HIGHEST


def shift_lanes(values, amount):
    amount = amount % LANES
    return values if amount == 0 else pltpu.roll(values, amount, 1)


def kernel(
    counts, dims, res_ref, dir_ref, pow_ref, gram_ref, proj_ref,
    v_ref, t_ref, ysend, yrecv, zsend, zrecv, xsend, xrecv,
    red0, red1, red2,
    ys_sem, yr_sem, zs_sem, zr_sem, xs_sem, xr_sem,
    s0_sem, r0_sem, s1_sem, r1_sem, s2_sem, r2_sem,
):
    nx, ny, nz = counts
    cx, cy, cz = dims
    pitch = cy + 4
    rows = cz + 16
    gx, gy, gz = lax.axis_index("gx"), lax.axis_index("gy"), lax.axis_index("gz")
    here = {"gx": gx, "gy": gy, "gz": gz}
    size = {"gx": nx, "gy": ny, "gz": nz}

    def exists(offset):
        ok = None
        for axis, step in offset.items():
            if step == 0:
                continue
            test = here[axis] + step >= 0 if step < 0 else here[axis] + step < size[axis]
            ok = test if ok is None else jnp.logical_and(ok, test)
        return ok

    def target(offset):
        return {axis: here[axis] + step for axis, step in offset.items() if step != 0}

    yz_offsets = [{"gy": dy, "gz": dz} for dy in (-1, 0, 1) for dz in (-1, 1)]
    y_offsets = [{"gy": -1}, {"gy": 1}]
    x_offsets = [{"gx": -1}, {"gx": 1}]
    diagonals = [o for o in yz_offsets if o["gy"] != 0]

    barrier = pltpu.get_barrier_semaphore()
    expected = (nx - 1) + (ny - 1) + (nz - 1)
    for axis in ("gx", "gy", "gz"):
        for k in range(1, size[axis]):
            other = lax.rem(here[axis] + k, size[axis])
            pl.semaphore_signal(barrier, inc=1, device_id={axis: other}, device_id_type=MESH)
    for offset in diagonals:
        there = exists(offset)
        expected = expected + there.astype(jnp.int32)

        @pl.when(there)
        def _():
            pl.semaphore_signal(barrier, inc=1, device_id=target(offset), device_id_type=MESH)

    lane = lax.broadcasted_iota(jnp.int32, (rows, LANES), 1)
    row = lax.broadcasted_iota(jnp.int32, (rows, LANES), 0)
    slot_x = lane // pitch
    slot_y = lane - slot_x * pitch
    at_x, at_y, at_z = slot_x - 1, slot_y - 2, row - 8
    own = (at_x >= 0) & (at_x < cx) & (at_y >= 0) & (at_y < cy) & (at_z >= 0) & (at_z < cz)
    sub = (
        (at_x >= -1) & (at_x <= cx) & (at_y >= -1) & (at_y <= cy) & (at_z >= -1) & (at_z <= cz)
        & (gx * cx + at_x >= 0) & (gx * cx + at_x < nx * cx)
        & (gy * cy + at_y >= 0) & (gy * cy + at_y < ny * cy)
        & (gz * cz + at_z >= 0) & (gz * cz + at_z < nz * cz)
    )

    pick_cell = lax.broadcasted_iota(jnp.int32, (cx * cy, LANES), 0)
    pick_lane = lax.broadcasted_iota(jnp.int32, (cx * cy, LANES), 1)
    pick = (pick_lane == (pick_cell // cy + 1) * pitch + pick_cell % cy + 2).astype(jnp.float32)

    def spread(block_ref):
        flat = block_ref[...].reshape(cx * cy, cz)
        return lax.dot_general(
            flat, pick, (((0,), (0,)), ((), ())), precision=HIGHEST,
            preferred_element_type=jnp.float32,
        )

    def collect(field):
        flat = lax.dot_general(
            pick, field, (((1,), (1,)), ((), ())), precision=HIGHEST,
            preferred_element_type=jnp.float32,
        )
        return flat.reshape(cx, cy, cz)

    def neighbours(u):
        return (
            jnp.where(lane >= pitch, shift_lanes(u, pitch), 0.0)
            + jnp.where(lane < cx * pitch + pitch, shift_lanes(u, -pitch), 0.0) + shift_lanes(u, 1) + shift_lanes(u, -1)
            + pltpu.roll(u, 1, 0) + pltpu.roll(u, rows - 1, 0)
        )

    edge = jnp.zeros((8, LANES), jnp.float32)
    residual_rows = spread(res_ref)
    u0 = jnp.concatenate([edge, spread(dir_ref), edge], axis=0)
    u1 = jnp.concatenate([edge, residual_rows, edge], axis=0)
    v_ref[2 * STEPS + 1] = residual_rows
    t_ref[...] = jnp.zeros_like(t_ref)
    for index, offset in enumerate(y_offsets):
        @pl.when(jnp.logical_not(exists({"gy": -offset["gy"]})))
        def _():
            for r in range(STEPS + 1):
                yrecv[r, index] = jnp.zeros((rows, LANES), jnp.float32)
    for index, offset in enumerate(x_offsets):
        @pl.when(jnp.logical_not(exists({"gx": -offset["gx"]})))
        def _():
            for r in range(STEPS + 1):
                xrecv[r, index] = jnp.zeros((rows, LANES), jnp.float32)
    for index, offset in enumerate(yz_offsets):
        @pl.when(jnp.logical_not(exists({k: -s for k, s in offset.items()})))
        def _():
            for r in range(STEPS + 1):
                zrecv[r, index] = jnp.zeros((8, LANES), jnp.float32)

    pl.semaphore_wait(barrier, expected)

    def copy_y(r, index):
        return pltpu.make_async_remote_copy(
            ysend.at[r, index], yrecv.at[r, index], ys_sem.at[r, index], yr_sem.at[r, index],
            device_id=target(y_offsets[index]), device_id_type=MESH)

    def copy_x(r, index):
        return pltpu.make_async_remote_copy(
            xsend.at[r, index], xrecv.at[r, index], xs_sem.at[r, index], xr_sem.at[r, index],
            device_id=target(x_offsets[index]), device_id_type=MESH)

    def copy_z(r, index):
        side = 0 if yz_offsets[index]["gz"] < 0 else 1
        return pltpu.make_async_remote_copy(
            zsend.at[r, side], zrecv.at[r, index], zs_sem.at[r, index], zr_sem.at[r, index],
            device_id=target(yz_offsets[index]), device_id_type=MESH)

    def start(make, r, offsets):
        for index, offset in enumerate(offsets):
            @pl.when(exists(offset))
            def _():
                make(r, index).start()

    def wait(make, r, offsets):
        for index, offset in enumerate(offsets):
            @pl.when(exists({k: -s for k, s in offset.items()}))
            def _():
                make(r, index).wait_recv()

    def wait_sent(make, r, offsets):
        for index, offset in enumerate(offsets):
            @pl.when(exists(offset))
            def _():
                make(r, index).wait_send()

    def dot_rows(a, b):
        return jnp.sum(a * b, axis=0, keepdims=True)

    total = 2 * STEPS + 1
    pending = None

    def account(r, images):
        fresh = [r] + ([STEPS + r] if r > 0 else [])
        done = list(range(r + 1)) + [STEPS + 1 + k for k in range(r)]
        for a in fresh:
            image = images[0] if a == r else images[1]
            for b in done:
                if a == r and b == STEPS + r and r > 0:
                    continue
                part = dot_rows(v_ref[b], image)
                t_ref[pl.ds(a * total + b, 1), :] = part
                if a != b:
                    t_ref[pl.ds(b * total + a, 1), :] = part
            t_ref[pl.ds(total * total + a, 1), :] = dot_rows(v_ref[a], v_ref[total])

    def emit(r):
        if r > 0:
            pow_ref[0, r - 1] = collect(v_ref[r])
            pow_ref[1, r - 1] = collect(v_ref[STEPS + r])

    low = lambda v: jnp.where(slot_y < 3, v, 0.0)
    span = lambda start_lane, stop_lane: (lane >= start_lane) & (lane < stop_lane)
    top = cx * pitch
    for r in range(STEPS + 1):
        for side, head in ((0, 7), (1, cz + 6)):
            zsend[r, side] = jnp.concatenate(
                [u0[head:head + 3], u1[head:head + 3], jnp.zeros((2, LANES), jnp.float32)], axis=0)
        ysend[r, 0] = jnp.where(slot_y >= 9, shift_lanes(u0, cy), shift_lanes(u1, cy - 3))
        ysend[r, 1] = jnp.where(slot_y < 3, shift_lanes(u0, -cy), shift_lanes(u1, 3 - cy))
        start(copy_z, r, yz_offsets)
        start(copy_y, r, y_offsets)
        if pending is not None:
            account(r - 1, pending)
            emit(r - 1)
        wait(copy_y, r, y_offsets)
        from_above, from_below = yrecv[r, 0], yrecv[r, 1]
        p0 = u0 + jnp.where(slot_y >= 9, from_above, 0.0) + low(from_below)
        p1 = (
            u1 + jnp.where(slot_y >= 9, shift_lanes(from_above, 3), 0.0)
            + low(shift_lanes(from_below, -3))
        )
        wait(copy_z, r, yz_offsets)
        tile_slot = slot_y[:8]
        tiles = []
        for side in (0, 1):
            mid = zrecv[r, 2 + side]
            down = jnp.where(tile_slot >= 9, shift_lanes(zrecv[r, side], cy), 0.0)
            up = jnp.where(tile_slot < 3, shift_lanes(zrecv[r, 4 + side], -cy), 0.0)
            tiles.append(mid + down + up)

        def with_tiles(p, first):
            upper, lower = tiles[0][first:first + 3], tiles[1][first:first + 3]
            zero = lambda n: jnp.zeros((n, LANES), jnp.float32)
            head = p[:16] + jnp.concatenate([zero(6), lower, zero(7)], axis=0)
            tail = p[rows - 16:] + jnp.concatenate([zero(7), upper, zero(6)], axis=0)
            return jnp.concatenate([head, p[16:rows - 16], tail], axis=0)

        p0, p1 = with_tiles(p0, 0), with_tiles(p1, 3)
        width = 3 * pitch
        xsend[r, 0] = jnp.where(lane < width, p0, shift_lanes(p1, width))
        far = (cx - 1) * pitch
        xsend[r, 1] = jnp.where(lane < width, shift_lanes(p0, -far), shift_lanes(p1, width - far))
        start(copy_x, r, x_offsets)
        wait(copy_x, r, x_offsets)
        beyond, before = xrecv[r, 0], xrecv[r, 1]
        at_low, at_high = span(0, 2 * pitch), span(top, top + 2 * pitch)
        ext_low, ext_high = span(0, pitch), span(top + pitch, top + 2 * pitch)

        def with_x(p, first):
            main = (
                p + jnp.where(at_low, shift_lanes(before, -first - pitch), 0.0)
                + jnp.where(at_high, shift_lanes(beyond, top - first), 0.0)
            )
            far_cells = (
                jnp.where(ext_low, shift_lanes(before, -first), 0.0)
                + jnp.where(ext_high, shift_lanes(beyond, top - pitch - first), 0.0)
            )
            return main, far_cells

        p0, far0 = with_x(p0, 0)
        p1, far1 = with_x(p1, width)
        p0 = jnp.where(lane < top + 2 * pitch, p0, 0.0)
        p1 = jnp.where(lane < top + 2 * pitch, p1, 0.0)
        b0 = jnp.where(sub, 6.0 * p0 - neighbours(p0) - far0, 0.0)
        a1 = jnp.where(sub, 6.0 * p1 - neighbours(p1) - far1, 0.0)
        b1 = jnp.where(sub, p1, 0.0) if r == 0 else a1
        v_ref[r] = jnp.where(own, p0, 0.0)[8:8 + cz]
        if r > 0:
            v_ref[STEPS + r] = jnp.where(own, p1, 0.0)[8:8 + cz]
        pending = (b0[8:8 + cz], a1[8:8 + cz])
        if r < STEPS:
            c0, c1 = b0 * (1.0 / 9.0), b1 * (1.0 / 9.0)
            u0, u1 = c0, c1
            for _ in range(SWEEPS - 1):
                u0 = jnp.where(sub, c0 + u0 * (1.0 / 3.0) + neighbours(u0) * (1.0 / 9.0), 0.0)
                u1 = jnp.where(sub, c1 + u1 * (1.0 / 3.0) + neighbours(u1) * (1.0 / 9.0), 0.0)

    account(STEPS, pending)
    value = lax.dot_general(
        jnp.ones((8, LANES), jnp.float32), t_ref[...], (((1,), (1,)), ((), ())),
        precision=HIGHEST, preferred_element_type=jnp.float32)

    def gather(value, axis, buffer, s_sem, r_sem, first):
        me, n = here[axis], size[axis]
        buffer[0] = value
        def make(k):
            return pltpu.make_async_remote_copy(
                buffer.at[0], buffer.at[k], s_sem.at[k], r_sem.at[k],
                device_id={axis: lax.rem(me + k, n)}, device_id_type=MESH)
        for k in range(1, n):
            make(k).start()
        if first:
            emit(STEPS)
        for k in range(1, n):
            make(k).wait_recv()
        result = jnp.zeros_like(value)
        for g in range(n):
            result = result + buffer[lax.rem(me + n - g, n)]
        for k in range(1, n):
            make(k).wait_send()
        return result

    value = gather(value, "gy", red0, s0_sem, r0_sem, True)
    value = gather(value, "gx", red1, s1_sem, r1_sem, False)
    value = gather(value, "gz", red2, s2_sem, r2_sem, False)
    value = value * (1.0 / (nx * cx * ny * cy * nz * cz))
    for a in range(total):
        gram_ref[a:a + 1, :] = value[0:1, a * total:(a + 1) * total]
    proj_ref[...] = value[0:1, total * total:total * total + total]
    for r in range(STEPS + 1):
        wait_sent(copy_y, r, y_offsets)
        wait_sent(copy_z, r, yz_offsets)
        wait_sent(copy_x, r, x_offsets)


def solution(mesh):
    counts = tuple(mesh.shape[a] for a in ("gx", "gy", "gz"))

    def local(residual, direction):
        dims = residual.shape
        rows = dims[2] + 16
        total = 2 * STEPS + 1
        rounds = STEPS + 1
        f32 = jnp.float32
        dma = pltpu.SemaphoreType.DMA
        vm = pl.BlockSpec(memory_space=pltpu.VMEM)
        powers, gram, proj = pl.pallas_call(
            functools.partial(kernel, counts, dims),
            out_shape=(
                jax.ShapeDtypeStruct((2, STEPS) + dims, f32),
                jax.ShapeDtypeStruct((total, total), f32),
                jax.ShapeDtypeStruct((1, total), f32),
            ),
            in_specs=[vm, vm],
            out_specs=(vm, vm, vm),
            scratch_shapes=[
                pltpu.VMEM((total + 1, dims[2], LANES), f32),
                pltpu.VMEM((LANES, LANES), f32),
                pltpu.VMEM((rounds, 2, rows, LANES), f32),
                pltpu.VMEM((rounds, 2, rows, LANES), f32),
                pltpu.VMEM((rounds, 2, 8, LANES), f32),
                pltpu.VMEM((rounds, 6, 8, LANES), f32),
                pltpu.VMEM((rounds, 2, rows, LANES), f32),
                pltpu.VMEM((rounds, 2, rows, LANES), f32),
                pltpu.VMEM((counts[1], 8, LANES), f32),
                pltpu.VMEM((counts[0], 8, LANES), f32),
                pltpu.VMEM((counts[2], 8, LANES), f32),
                dma((rounds, 2)), dma((rounds, 2)),
                dma((rounds, 6)), dma((rounds, 6)),
                dma((rounds, 2)), dma((rounds, 2)),
                dma((counts[1],)), dma((counts[1],)),
                dma((counts[0],)), dma((counts[0],)),
                dma((counts[2],)), dma((counts[2],)),
            ],
            compiler_params=pltpu.CompilerParams(collective_id=0, has_side_effects=True),
            name="powers_basis",
        )(residual, direction)
        return powers, gram, proj.reshape(total)

    placed = (P("gx", "gy", "gz"), P("gx", "gy", "gz"))
    return jax.shard_map(
        local,
        mesh=mesh,
        in_specs=placed,
        out_specs=(P(None, None, "gx", "gy", "gz"), P(), P()),
        check_vma=False,
    )
```

```python
import functools

import jax
import jax.numpy as jnp
from jax import lax
from jax.experimental import pallas as pl
from jax.experimental.pallas import tpu as pltpu
from jax.sharding import PartitionSpec as P

STEPS = 4
SWEEPS = 3
LANES = 128
MESH = pl.DeviceIdType.MESH
HIGHEST = lax.Precision.HIGHEST


def shift_lanes(values, amount):
    amount = amount % LANES
    return values if amount == 0 else pltpu.roll(values, amount, 1)


def kernel(
    counts, dims, res_ref, dir_ref, pow_ref, gram_ref, proj_ref,
    v_ref, t_ref, ysend, yrecv, zsend, zrecv, xsend, xrecv,
    red0, red1,
    ys_sem, yr_sem, zs_sem, zr_sem, xs_sem, xr_sem,
    s0_sem, r0_sem, s1_sem, r1_sem,
):
    nx, ny, nz = counts
    cx, cy, cz = dims
    pitch = cy + 4
    rows = cz + 16
    gx, gy, gz = lax.axis_index("gx"), lax.axis_index("gy"), lax.axis_index("gz")
    here = {"gx": gx, "gy": gy, "gz": gz}
    size = {"gx": nx, "gy": ny, "gz": nz}

    def exists(offset):
        ok = None
        for axis, step in offset.items():
            if step == 0:
                continue
            test = here[axis] + step >= 0 if step < 0 else here[axis] + step < size[axis]
            ok = test if ok is None else jnp.logical_and(ok, test)
        return ok

    def target(offset):
        return {axis: here[axis] + step for axis, step in offset.items() if step != 0}

    yz_offsets = [{"gy": dy, "gz": dz} for dy in (-1, 0, 1) for dz in (-1, 1)]
    y_offsets = [{"gy": -1}, {"gy": 1}]
    x_offsets = [{"gx": -1}, {"gx": 1}]

    barrier = pltpu.get_barrier_semaphore()
    expected = (nx - 1) + (ny * nz - 1)

    def in_line(k):
        return {"gx": lax.rem(gx + k, nx)}

    def in_plane(k):
        ky, kz = divmod(k, nz)
        place = {}
        if ky:
            place["gy"] = lax.rem(gy + ky, ny)
        if kz:
            place["gz"] = lax.rem(gz + kz, nz)
        return place

    for count, place in ((nx, in_line), (ny * nz, in_plane)):
        for k in range(1, count):
            pl.semaphore_signal(barrier, inc=1, device_id=place(k), device_id_type=MESH)

    lane = lax.broadcasted_iota(jnp.int32, (rows, LANES), 1)
    row = lax.broadcasted_iota(jnp.int32, (rows, LANES), 0)
    slot_x = lane // pitch
    slot_y = lane - slot_x * pitch
    at_x, at_y, at_z = slot_x - 1, slot_y - 2, row - 8
    own = (at_x >= 0) & (at_x < cx) & (at_y >= 0) & (at_y < cy) & (at_z >= 0) & (at_z < cz)
    sub = (
        (at_x >= -1) & (at_x <= cx) & (at_y >= -1) & (at_y <= cy) & (at_z >= -1) & (at_z <= cz)
        & (gx * cx + at_x >= 0) & (gx * cx + at_x < nx * cx)
        & (gy * cy + at_y >= 0) & (gy * cy + at_y < ny * cy)
        & (gz * cz + at_z >= 0) & (gz * cz + at_z < nz * cz)
    )

    pick_cell = lax.broadcasted_iota(jnp.int32, (cx * cy, LANES), 0)
    pick_lane = lax.broadcasted_iota(jnp.int32, (cx * cy, LANES), 1)
    pick = (pick_lane == (pick_cell // cy + 1) * pitch + pick_cell % cy + 2).astype(jnp.float32)

    def spread(block_ref):
        flat = block_ref[...].reshape(cx * cy, cz)
        return lax.dot_general(
            flat, pick, (((0,), (0,)), ((), ())), precision=HIGHEST,
            preferred_element_type=jnp.float32,
        )

    def collect(field):
        flat = lax.dot_general(
            pick, field, (((1,), (1,)), ((), ())), precision=HIGHEST,
            preferred_element_type=jnp.float32,
        )
        return flat.reshape(cx, cy, cz)

    def neighbours(u):
        return (
            jnp.where(lane >= pitch, shift_lanes(u, pitch), 0.0)
            + jnp.where(lane < cx * pitch + pitch, shift_lanes(u, -pitch), 0.0) + shift_lanes(u, 1) + shift_lanes(u, -1)
            + pltpu.roll(u, 1, 0) + pltpu.roll(u, rows - 1, 0)
        )

    edge = jnp.zeros((8, LANES), jnp.float32)
    residual_rows = spread(res_ref)
    u0 = jnp.concatenate([edge, spread(dir_ref), edge], axis=0)
    u1 = jnp.concatenate([edge, residual_rows, edge], axis=0)
    v_ref[2 * STEPS + 1] = residual_rows
    t_ref[...] = jnp.zeros_like(t_ref)
    for index, offset in enumerate(y_offsets):
        @pl.when(jnp.logical_not(exists({"gy": -offset["gy"]})))
        def _():
            for r in range(STEPS + 1):
                yrecv[r, index] = jnp.zeros((rows, LANES), jnp.float32)
    for index, offset in enumerate(x_offsets):
        @pl.when(jnp.logical_not(exists({"gx": -offset["gx"]})))
        def _():
            for r in range(STEPS + 1):
                xrecv[r, index] = jnp.zeros((rows, LANES), jnp.float32)
    for index, offset in enumerate(yz_offsets):
        @pl.when(jnp.logical_not(exists({k: -s for k, s in offset.items()})))
        def _():
            for r in range(STEPS + 1):
                zrecv[r, index] = jnp.zeros((8, LANES), jnp.float32)

    pl.semaphore_wait(barrier, expected)

    def copy_y(r, index):
        return pltpu.make_async_remote_copy(
            ysend.at[r, index], yrecv.at[r, index], ys_sem.at[r, index], yr_sem.at[r, index],
            device_id=target(y_offsets[index]), device_id_type=MESH)

    def copy_x(r, index):
        return pltpu.make_async_remote_copy(
            xsend.at[r, index], xrecv.at[r, index], xs_sem.at[r, index], xr_sem.at[r, index],
            device_id=target(x_offsets[index]), device_id_type=MESH)

    def copy_z(r, index):
        side = 0 if yz_offsets[index]["gz"] < 0 else 1
        return pltpu.make_async_remote_copy(
            zsend.at[r, side], zrecv.at[r, index], zs_sem.at[r, index], zr_sem.at[r, index],
            device_id=target(yz_offsets[index]), device_id_type=MESH)

    def start(make, r, offsets):
        for index, offset in enumerate(offsets):
            @pl.when(exists(offset))
            def _():
                make(r, index).start()

    def wait(make, r, offsets):
        for index, offset in enumerate(offsets):
            @pl.when(exists({k: -s for k, s in offset.items()}))
            def _():
                make(r, index).wait_recv()

    def wait_sent(make, r, offsets):
        for index, offset in enumerate(offsets):
            @pl.when(exists(offset))
            def _():
                make(r, index).wait_send()

    def dot_rows(a, b):
        return jnp.sum(a * b, axis=0, keepdims=True)

    total = 2 * STEPS + 1
    pending = None

    def account(r, images):
        fresh = [r] + ([STEPS + r] if r > 0 else [])
        done = list(range(r + 1)) + [STEPS + 1 + k for k in range(r)]
        for a in fresh:
            image = images[0] if a == r else images[1]
            for b in done:
                if a == r and b == STEPS + r and r > 0:
                    continue
                part = dot_rows(v_ref[b], image)
                t_ref[pl.ds(a * total + b, 1), :] = part
                if a != b:
                    t_ref[pl.ds(b * total + a, 1), :] = part
            t_ref[pl.ds(total * total + a, 1), :] = dot_rows(v_ref[a], v_ref[total])

    def emit(r):
        if r > 0:
            pow_ref[0, r - 1] = collect(v_ref[r])
            pow_ref[1, r - 1] = collect(v_ref[STEPS + r])

    low = lambda v: jnp.where(slot_y < 3, v, 0.0)
    span = lambda start_lane, stop_lane: (lane >= start_lane) & (lane < stop_lane)
    top = cx * pitch
    for r in range(STEPS + 1):
        for side, head in ((0, 7), (1, cz + 6)):
            zsend[r, side] = jnp.concatenate(
                [u0[head:head + 3], u1[head:head + 3], jnp.zeros((2, LANES), jnp.float32)], axis=0)
        ysend[r, 0] = jnp.where(slot_y >= 9, shift_lanes(u0, cy), shift_lanes(u1, cy - 3))
        ysend[r, 1] = jnp.where(slot_y < 3, shift_lanes(u0, -cy), shift_lanes(u1, 3 - cy))
        start(copy_z, r, yz_offsets)
        start(copy_y, r, y_offsets)
        if pending is not None:
            account(r - 1, pending)
        wait(copy_y, r, y_offsets)
        from_above, from_below = yrecv[r, 0], yrecv[r, 1]
        p0 = u0 + jnp.where(slot_y >= 9, from_above, 0.0) + low(from_below)
        p1 = (
            u1 + jnp.where(slot_y >= 9, shift_lanes(from_above, 3), 0.0)
            + low(shift_lanes(from_below, -3))
        )
        wait(copy_z, r, yz_offsets)
        tile_slot = slot_y[:8]
        tiles = []
        for side in (0, 1):
            mid = zrecv[r, 2 + side]
            down = jnp.where(tile_slot >= 9, shift_lanes(zrecv[r, side], cy), 0.0)
            up = jnp.where(tile_slot < 3, shift_lanes(zrecv[r, 4 + side], -cy), 0.0)
            tiles.append(mid + down + up)

        def with_tiles(p, first):
            upper, lower = tiles[0][first:first + 3], tiles[1][first:first + 3]
            zero = lambda n: jnp.zeros((n, LANES), jnp.float32)
            head = p[:16] + jnp.concatenate([zero(6), lower, zero(7)], axis=0)
            tail = p[rows - 16:] + jnp.concatenate([zero(7), upper, zero(6)], axis=0)
            return jnp.concatenate([head, p[16:rows - 16], tail], axis=0)

        p0, p1 = with_tiles(p0, 0), with_tiles(p1, 3)
        width = 3 * pitch
        xsend[r, 0] = jnp.where(lane < width, p0, shift_lanes(p1, width))
        far = (cx - 1) * pitch
        xsend[r, 1] = jnp.where(lane < width, shift_lanes(p0, -far), shift_lanes(p1, width - far))
        start(copy_x, r, x_offsets)
        if r > 0:
            emit(r - 1)
        wait(copy_x, r, x_offsets)
        beyond, before = xrecv[r, 0], xrecv[r, 1]
        at_low, at_high = span(0, 2 * pitch), span(top, top + 2 * pitch)
        ext_low, ext_high = span(0, pitch), span(top + pitch, top + 2 * pitch)

        def with_x(p, first):
            main = (
                p + jnp.where(at_low, shift_lanes(before, -first - pitch), 0.0)
                + jnp.where(at_high, shift_lanes(beyond, top - first), 0.0)
            )
            far_cells = (
                jnp.where(ext_low, shift_lanes(before, -first), 0.0)
                + jnp.where(ext_high, shift_lanes(beyond, top - pitch - first), 0.0)
            )
            return main, far_cells

        p0, far0 = with_x(p0, 0)
        p1, far1 = with_x(p1, width)
        p0 = jnp.where(lane < top + 2 * pitch, p0, 0.0)
        p1 = jnp.where(lane < top + 2 * pitch, p1, 0.0)
        b0 = jnp.where(sub, 6.0 * p0 - neighbours(p0) - far0, 0.0)
        a1 = jnp.where(sub, 6.0 * p1 - neighbours(p1) - far1, 0.0)
        b1 = jnp.where(sub, p1, 0.0) if r == 0 else a1
        v_ref[r] = jnp.where(own, p0, 0.0)[8:8 + cz]
        if r > 0:
            v_ref[STEPS + r] = jnp.where(own, p1, 0.0)[8:8 + cz]
        pending = (b0[8:8 + cz], a1[8:8 + cz])
        if r < STEPS:
            c0, c1 = b0 * (1.0 / 9.0), b1 * (1.0 / 9.0)
            u0, u1 = c0, c1
            for _ in range(SWEEPS - 1):
                u0 = jnp.where(sub, c0 + u0 * (1.0 / 3.0) + neighbours(u0) * (1.0 / 9.0), 0.0)
                u1 = jnp.where(sub, c1 + u1 * (1.0 / 3.0) + neighbours(u1) * (1.0 / 9.0), 0.0)

    account(STEPS, pending)
    value = lax.dot_general(
        jnp.ones((8, LANES), jnp.float32), t_ref[...], (((1,), (1,)), ((), ())),
        precision=HIGHEST, preferred_element_type=jnp.float32)

    def gather(value, count, place, slots, buffer, s_sem, r_sem, first):
        buffer[0] = value

        def make(k):
            return pltpu.make_async_remote_copy(
                buffer.at[0], buffer.at[k], s_sem.at[k], r_sem.at[k],
                device_id=place(k), device_id_type=MESH)

        for k in range(1, count):
            make(k).start()
        if first:
            emit(STEPS)
        for k in range(1, count):
            make(k).wait_recv()
        result = jnp.zeros_like(value)
        for slot in slots:
            result = result + buffer[slot]
        for k in range(1, count):
            make(k).wait_send()
        return result

    plane_slots = [
        lax.rem(gy + ny - g, ny) * nz + lax.rem(gz + nz - h, nz)
        for g in range(ny) for h in range(nz)
    ]
    line_slots = [lax.rem(gx + nx - g, nx) for g in range(nx)]
    value = gather(value, ny * nz, in_plane, plane_slots, red0, s0_sem, r0_sem, True)
    value = gather(value, nx, in_line, line_slots, red1, s1_sem, r1_sem, False)
    value = value * (1.0 / (nx * cx * ny * cy * nz * cz))
    for a in range(total):
        gram_ref[a:a + 1, :] = value[0:1, a * total:(a + 1) * total]
    proj_ref[...] = value[0:1, total * total:total * total + total]
    for r in range(STEPS + 1):
        wait_sent(copy_y, r, y_offsets)
        wait_sent(copy_z, r, yz_offsets)
        wait_sent(copy_x, r, x_offsets)


def solution(mesh):
    counts = tuple(mesh.shape[a] for a in ("gx", "gy", "gz"))

    def local(residual, direction):
        dims = residual.shape
        rows = dims[2] + 16
        total = 2 * STEPS + 1
        rounds = STEPS + 1
        f32 = jnp.float32
        dma = pltpu.SemaphoreType.DMA
        vm = pl.BlockSpec(memory_space=pltpu.VMEM)
        powers, gram, proj = pl.pallas_call(
            functools.partial(kernel, counts, dims),
            out_shape=(
                jax.ShapeDtypeStruct((2, STEPS) + dims, f32),
                jax.ShapeDtypeStruct((total, total), f32),
                jax.ShapeDtypeStruct((1, total), f32),
            ),
            in_specs=[vm, vm],
            out_specs=(vm, vm, vm),
            scratch_shapes=[
                pltpu.VMEM((total + 1, dims[2], LANES), f32),
                pltpu.VMEM((LANES, LANES), f32),
                pltpu.VMEM((rounds, 2, rows, LANES), f32),
                pltpu.VMEM((rounds, 2, rows, LANES), f32),
                pltpu.VMEM((rounds, 2, 8, LANES), f32),
                pltpu.VMEM((rounds, 6, 8, LANES), f32),
                pltpu.VMEM((rounds, 2, rows, LANES), f32),
                pltpu.VMEM((rounds, 2, rows, LANES), f32),
                pltpu.VMEM((counts[1] * counts[2], 8, LANES), f32),
                pltpu.VMEM((counts[0], 8, LANES), f32),
                dma((rounds, 2)), dma((rounds, 2)),
                dma((rounds, 6)), dma((rounds, 6)),
                dma((rounds, 2)), dma((rounds, 2)),
                dma((counts[1] * counts[2],)), dma((counts[1] * counts[2],)),
                dma((counts[0],)), dma((counts[0],)),
            ],
            compiler_params=pltpu.CompilerParams(collective_id=0, has_side_effects=True),
            name="powers_basis",
        )(residual, direction)
        return powers, gram, proj.reshape(total)

    placed = (P("gx", "gy", "gz"), P("gx", "gy", "gz"))
    return jax.shard_map(
        local,
        mesh=mesh,
        in_specs=placed,
        out_specs=(P(None, None, "gx", "gy", "gz"), P(), P()),
        check_vma=False,
    )
```

```python
import functools

import jax
import jax.numpy as jnp
from jax import lax
from jax.experimental import pallas as pl
from jax.experimental.pallas import tpu as pltpu
from jax.sharding import PartitionSpec as P

STEPS = 4
SWEEPS = 3
LANES = 128
MESH = pl.DeviceIdType.MESH
HIGHEST = lax.Precision.HIGHEST


def shift_lanes(values, amount):
    amount = amount % LANES
    return values if amount == 0 else pltpu.roll(values, amount, 1)


def kernel(
    counts, dims, res_ref, dir_ref, pow_ref, gram_ref, proj_ref,
    v_ref, t_ref, ysend, yrecv, zsend, zrecv, xsend, xrecv,
    red0, red1,
    ys_sem, yr_sem, zs_sem, zr_sem, xs_sem, xr_sem,
    s0_sem, r0_sem, s1_sem, r1_sem,
):
    nx, ny, nz = counts
    cx, cy, cz = dims
    pitch = cy + 4
    rows = cz + 16
    gx, gy, gz = lax.axis_index("gx"), lax.axis_index("gy"), lax.axis_index("gz")
    here = {"gx": gx, "gy": gy, "gz": gz}
    size = {"gx": nx, "gy": ny, "gz": nz}

    def exists(offset):
        ok = None
        for axis, step in offset.items():
            if step == 0:
                continue
            test = here[axis] + step >= 0 if step < 0 else here[axis] + step < size[axis]
            ok = test if ok is None else jnp.logical_and(ok, test)
        return ok

    def target(offset):
        return {axis: here[axis] + step for axis, step in offset.items() if step != 0}

    yz_offsets = [{"gy": dy, "gz": dz} for dy in (-1, 0, 1) for dz in (-1, 1)]
    y_offsets = [{"gy": -1}, {"gy": 1}]
    x_offsets = [{"gx": -1}, {"gx": 1}]

    barrier = pltpu.get_barrier_semaphore()
    expected = (nx - 1) + (ny * nz - 1)

    def in_line(k):
        return {"gx": lax.rem(gx + k, nx)}

    def in_plane(k):
        ky, kz = divmod(k, nz)
        place = {}
        if ky:
            place["gy"] = lax.rem(gy + ky, ny)
        if kz:
            place["gz"] = lax.rem(gz + kz, nz)
        return place

    for count, place in ((nx, in_line), (ny * nz, in_plane)):
        for k in range(1, count):
            pl.semaphore_signal(barrier, inc=1, device_id=place(k), device_id_type=MESH)

    lane = lax.broadcasted_iota(jnp.int32, (1, LANES), 1)
    row = lax.broadcasted_iota(jnp.int32, (rows, LANES), 0)
    slot_x = lane // pitch
    slot_y = lane - slot_x * pitch
    at_x, at_y, at_z = slot_x - 1, slot_y - 2, row - 8
    own = (at_x >= 0) & (at_x < cx) & (at_y >= 0) & (at_y < cy) & (at_z >= 0) & (at_z < cz)
    sub = (
        (at_x >= -1) & (at_x <= cx) & (at_y >= -1) & (at_y <= cy) & (at_z >= -1) & (at_z <= cz)
        & (gx * cx + at_x >= 0) & (gx * cx + at_x < nx * cx)
        & (gy * cy + at_y >= 0) & (gy * cy + at_y < ny * cy)
        & (gz * cz + at_z >= 0) & (gz * cz + at_z < nz * cz)
    )

    pick_cell = lax.broadcasted_iota(jnp.int32, (cx * cy, LANES), 0)
    pick_lane = lax.broadcasted_iota(jnp.int32, (cx * cy, LANES), 1)
    pick = (pick_lane == (pick_cell // cy + 1) * pitch + pick_cell % cy + 2).astype(jnp.float32)

    def spread(block_ref):
        flat = block_ref[...].reshape(cx * cy, cz)
        return lax.dot_general(
            flat, pick, (((0,), (0,)), ((), ())), precision=HIGHEST,
            preferred_element_type=jnp.float32,
        )

    def collect(field):
        flat = lax.dot_general(
            pick, field, (((1,), (1,)), ((), ())), precision=HIGHEST,
            preferred_element_type=jnp.float32,
        )
        return flat.reshape(cx, cy, cz)

    def neighbours(u):
        return (
            jnp.where(lane >= pitch, shift_lanes(u, pitch), 0.0)
            + jnp.where(lane < cx * pitch + pitch, shift_lanes(u, -pitch), 0.0) + shift_lanes(u, 1) + shift_lanes(u, -1)
            + pltpu.roll(u, 1, 0) + pltpu.roll(u, rows - 1, 0)
        )

    edge = jnp.zeros((8, LANES), jnp.float32)
    residual_rows = spread(res_ref)
    u0 = jnp.concatenate([edge, spread(dir_ref), edge], axis=0)
    u1 = jnp.concatenate([edge, residual_rows, edge], axis=0)
    v_ref[2 * STEPS + 1] = residual_rows
    t_ref[...] = jnp.zeros_like(t_ref)
    for index, offset in enumerate(y_offsets):
        @pl.when(jnp.logical_not(exists({"gy": -offset["gy"]})))
        def _():
            for r in range(STEPS + 1):
                yrecv[r, index] = jnp.zeros((rows, LANES), jnp.float32)
    for index, offset in enumerate(x_offsets):
        @pl.when(jnp.logical_not(exists({"gx": -offset["gx"]})))
        def _():
            for r in range(STEPS + 1):
                xrecv[r, index] = jnp.zeros((rows, LANES), jnp.float32)
    for index, offset in enumerate(yz_offsets):
        @pl.when(jnp.logical_not(exists({k: -s for k, s in offset.items()})))
        def _():
            for r in range(STEPS + 1):
                zrecv[r, index] = jnp.zeros((8, LANES), jnp.float32)

    pl.semaphore_wait(barrier, expected)

    def copy_y(r, index):
        return pltpu.make_async_remote_copy(
            ysend.at[r, index], yrecv.at[r, index], ys_sem.at[r, index], yr_sem.at[r, index],
            device_id=target(y_offsets[index]), device_id_type=MESH)

    def copy_x(r, index):
        return pltpu.make_async_remote_copy(
            xsend.at[r, index], xrecv.at[r, index], xs_sem.at[r, index], xr_sem.at[r, index],
            device_id=target(x_offsets[index]), device_id_type=MESH)

    def copy_z(r, index):
        side = 0 if yz_offsets[index]["gz"] < 0 else 1
        return pltpu.make_async_remote_copy(
            zsend.at[r, side], zrecv.at[r, index], zs_sem.at[r, index], zr_sem.at[r, index],
            device_id=target(yz_offsets[index]), device_id_type=MESH)

    def start(make, r, offsets):
        for index, offset in enumerate(offsets):
            @pl.when(exists(offset))
            def _():
                make(r, index).start()

    def wait(make, r, offsets):
        for index, offset in enumerate(offsets):
            @pl.when(exists({k: -s for k, s in offset.items()}))
            def _():
                make(r, index).wait_recv()

    def wait_sent(make, r, offsets):
        for index, offset in enumerate(offsets):
            @pl.when(exists(offset))
            def _():
                make(r, index).wait_send()

    def dot_rows(a, b):
        return jnp.sum(a * b, axis=0, keepdims=True)

    total = 2 * STEPS + 1
    pending = None

    def account(r, images):
        fresh = [r] + ([STEPS + r] if r > 0 else [])
        done = list(range(r + 1)) + [STEPS + 1 + k for k in range(r)]
        for a in fresh:
            image = images[0] if a == r else images[1]
            for b in done:
                if a == r and b == STEPS + r and r > 0:
                    continue
                part = dot_rows(v_ref[b], image)
                t_ref[pl.ds(a * total + b, 1), :] = part
                if a != b:
                    t_ref[pl.ds(b * total + a, 1), :] = part
            t_ref[pl.ds(total * total + a, 1), :] = dot_rows(v_ref[a], v_ref[total])

    def emit(r):
        if r > 0:
            pow_ref[0, r - 1] = collect(v_ref[r])
            pow_ref[1, r - 1] = collect(v_ref[STEPS + r])

    low = lambda v: jnp.where(slot_y < 3, v, 0.0)
    span = lambda start_lane, stop_lane: (lane >= start_lane) & (lane < stop_lane)
    top = cx * pitch
    for r in range(STEPS + 1):
        for side, head in ((0, 7), (1, cz + 6)):
            zsend[r, side] = jnp.concatenate(
                [u0[head:head + 3], u1[head:head + 3], jnp.zeros((2, LANES), jnp.float32)], axis=0)
        ysend[r, 0] = jnp.where(slot_y >= 9, shift_lanes(u0, cy), shift_lanes(u1, cy - 3))
        ysend[r, 1] = jnp.where(slot_y < 3, shift_lanes(u0, -cy), shift_lanes(u1, 3 - cy))
        start(copy_z, r, yz_offsets)
        start(copy_y, r, y_offsets)
        if pending is not None:
            account(r - 1, pending)
        wait(copy_y, r, y_offsets)
        from_above, from_below = yrecv[r, 0], yrecv[r, 1]
        p0 = u0 + jnp.where(slot_y >= 9, from_above, 0.0) + low(from_below)
        p1 = (
            u1 + jnp.where(slot_y >= 9, shift_lanes(from_above, 3), 0.0)
            + low(shift_lanes(from_below, -3))
        )
        wait(copy_z, r, yz_offsets)
        tile_slot = slot_y
        tiles = []
        for side in (0, 1):
            mid = zrecv[r, 2 + side]
            down = jnp.where(tile_slot >= 9, shift_lanes(zrecv[r, side], cy), 0.0)
            up = jnp.where(tile_slot < 3, shift_lanes(zrecv[r, 4 + side], -cy), 0.0)
            tiles.append(mid + down + up)

        def with_tiles(p, first):
            upper, lower = tiles[0][first:first + 3], tiles[1][first:first + 3]
            zero = lambda n: jnp.zeros((n, LANES), jnp.float32)
            head = p[:16] + jnp.concatenate([zero(6), lower, zero(7)], axis=0)
            tail = p[rows - 16:] + jnp.concatenate([zero(7), upper, zero(6)], axis=0)
            return jnp.concatenate([head, p[16:rows - 16], tail], axis=0)

        p0, p1 = with_tiles(p0, 0), with_tiles(p1, 3)
        width = 3 * pitch
        xsend[r, 0] = jnp.where(lane < width, p0, shift_lanes(p1, width))
        far = (cx - 1) * pitch
        xsend[r, 1] = jnp.where(lane < width, shift_lanes(p0, -far), shift_lanes(p1, width - far))
        start(copy_x, r, x_offsets)
        if r > 0:
            emit(r - 1)
        wait(copy_x, r, x_offsets)
        beyond, before = xrecv[r, 0], xrecv[r, 1]
        at_low, at_high = span(0, 2 * pitch), span(top, top + 2 * pitch)
        ext_low, ext_high = span(0, pitch), span(top + pitch, top + 2 * pitch)

        def with_x(p, first):
            main = (
                p + jnp.where(at_low, shift_lanes(before, -first - pitch), 0.0)
                + jnp.where(at_high, shift_lanes(beyond, top - first), 0.0)
            )
            far_cells = (
                jnp.where(ext_low, shift_lanes(before, -first), 0.0)
                + jnp.where(ext_high, shift_lanes(beyond, top - pitch - first), 0.0)
            )
            return main, far_cells

        p0, far0 = with_x(p0, 0)
        p1, far1 = with_x(p1, width)
        p0 = jnp.where(lane < top + 2 * pitch, p0, 0.0)
        p1 = jnp.where(lane < top + 2 * pitch, p1, 0.0)
        b0 = jnp.where(sub, 6.0 * p0 - neighbours(p0) - far0, 0.0)
        a1 = jnp.where(sub, 6.0 * p1 - neighbours(p1) - far1, 0.0)
        b1 = jnp.where(sub, p1, 0.0) if r == 0 else a1
        v_ref[r] = jnp.where(own, p0, 0.0)[8:8 + cz]
        if r > 0:
            v_ref[STEPS + r] = jnp.where(own, p1, 0.0)[8:8 + cz]
        pending = (b0[8:8 + cz], a1[8:8 + cz])
        if r < STEPS:
            c0, c1 = b0 * (1.0 / 9.0), b1 * (1.0 / 9.0)
            u0, u1 = c0, c1
            for _ in range(SWEEPS - 1):
                u0 = jnp.where(sub, c0 + u0 * (1.0 / 3.0) + neighbours(u0) * (1.0 / 9.0), 0.0)
                u1 = jnp.where(sub, c1 + u1 * (1.0 / 3.0) + neighbours(u1) * (1.0 / 9.0), 0.0)

    account(STEPS, pending)
    value = lax.dot_general(
        jnp.ones((8, LANES), jnp.float32), t_ref[...], (((1,), (1,)), ((), ())),
        precision=HIGHEST, preferred_element_type=jnp.float32)

    def gather(value, count, place, slots, buffer, s_sem, r_sem, first):
        buffer[0] = value

        def make(k):
            return pltpu.make_async_remote_copy(
                buffer.at[0], buffer.at[k], s_sem.at[k], r_sem.at[k],
                device_id=place(k), device_id_type=MESH)

        for k in range(1, count):
            make(k).start()
        if first:
            emit(STEPS)
        for k in range(1, count):
            make(k).wait_recv()
        result = jnp.zeros_like(value)
        for slot in slots:
            result = result + buffer[slot]
        for k in range(1, count):
            make(k).wait_send()
        return result

    plane_slots = [
        lax.rem(gy + ny - g, ny) * nz + lax.rem(gz + nz - h, nz)
        for g in range(ny) for h in range(nz)
    ]
    line_slots = [lax.rem(gx + nx - g, nx) for g in range(nx)]
    value = gather(value, ny * nz, in_plane, plane_slots, red0, s0_sem, r0_sem, True)
    value = gather(value, nx, in_line, line_slots, red1, s1_sem, r1_sem, False)
    value = value * (1.0 / (nx * cx * ny * cy * nz * cz))
    for a in range(total):
        gram_ref[a:a + 1, :] = value[0:1, a * total:(a + 1) * total]
    proj_ref[...] = value[0:1, total * total:total * total + total]
    for r in range(STEPS + 1):
        wait_sent(copy_y, r, y_offsets)
        wait_sent(copy_z, r, yz_offsets)
        wait_sent(copy_x, r, x_offsets)


def solution(mesh):
    counts = tuple(mesh.shape[a] for a in ("gx", "gy", "gz"))

    def local(residual, direction):
        dims = residual.shape
        rows = dims[2] + 16
        total = 2 * STEPS + 1
        rounds = STEPS + 1
        f32 = jnp.float32
        dma = pltpu.SemaphoreType.DMA
        vm = pl.BlockSpec(memory_space=pltpu.VMEM)
        powers, gram, proj = pl.pallas_call(
            functools.partial(kernel, counts, dims),
            out_shape=(
                jax.ShapeDtypeStruct((2, STEPS) + dims, f32),
                jax.ShapeDtypeStruct((total, total), f32),
                jax.ShapeDtypeStruct((1, total), f32),
            ),
            in_specs=[vm, vm],
            out_specs=(vm, vm, vm),
            scratch_shapes=[
                pltpu.VMEM((total + 1, dims[2], LANES), f32),
                pltpu.VMEM((LANES, LANES), f32),
                pltpu.VMEM((rounds, 2, rows, LANES), f32),
                pltpu.VMEM((rounds, 2, rows, LANES), f32),
                pltpu.VMEM((rounds, 2, 8, LANES), f32),
                pltpu.VMEM((rounds, 6, 8, LANES), f32),
                pltpu.VMEM((rounds, 2, rows, LANES), f32),
                pltpu.VMEM((rounds, 2, rows, LANES), f32),
                pltpu.VMEM((counts[1] * counts[2], 8, LANES), f32),
                pltpu.VMEM((counts[0], 8, LANES), f32),
                dma((rounds, 2)), dma((rounds, 2)),
                dma((rounds, 6)), dma((rounds, 6)),
                dma((rounds, 2)), dma((rounds, 2)),
                dma((counts[1] * counts[2],)), dma((counts[1] * counts[2],)),
                dma((counts[0],)), dma((counts[0],)),
            ],
            compiler_params=pltpu.CompilerParams(collective_id=0, has_side_effects=True),
            name="powers_basis",
        )(residual, direction)
        return powers, gram, proj.reshape(total)

    placed = (P("gx", "gy", "gz"), P("gx", "gy", "gz"))
    return jax.shard_map(
        local,
        mesh=mesh,
        in_specs=placed,
        out_specs=(P(None, None, "gx", "gy", "gz"), P(), P()),
        check_vma=False,
    )
```
